32 devices in a mesh: seq: 16 (over z, y, core), dp: 2 (over x).
Axes of the slice: x: 2, y: 2, z: 4, core: 2. Of those that a mesh axis runs over, the one named last changes fastest.
Arguments:
- q_student: bfloat16 [2, 8192, 1536], P('dp', 'seq'), may hold values from -8 to 8
- kv_student: bfloat16 [2, 128, 3072], P('dp', 'seq'), may hold values from -8 to 8
- q_target: bfloat16 [2, 8192, 1536], P('dp', 'seq'), may hold values from -8 to 8
- kv_target: bfloat16 [2, 128, 3072], P('dp', 'seq'), may hold values from -8 to 8
Outputs:
- student_out: bfloat16 [2, 8192, 1536], P('dp', 'seq')
- target_out: bfloat16 [2, 8192, 1536], P('dp', 'seq')
- distill_loss: float32 [], replicated
The draws below stay inside these ranges and needn't reach their ends.
All inputs are finite; a program needn't handle non-finite values.
Results may differ from the reference program's by a relative error of at most 0.004.
Values may be sent and summed in bfloat16 or wider, within the bound.
A program may use at most 128 MiB of HBM per device.

```python
import jax
import jax.numpy as jnp
from jax import lax

HEADS = 12
HD = 128
TOK_DEV = 512
TOKENS = 8192
KV_TOKENS = 128
CLIPS = 2
N_SEQ = 16


def draw_pairs(key, value_growth):
    feature_width = HEADS * HD
    key_list = jax.random.split(key, 7)
    clip_frac = jnp.arange(CLIPS).astype(jnp.float32)
    value_scale = 1.0 + value_growth * 1.5 * clip_frac
    queries = jnp.clip(2.5 * jax.random.normal(key_list[0], (CLIPS, TOKENS, feature_width), jnp.float32), -8.0, 8.0)
    key_part = jnp.clip(jax.random.normal(key_list[1], (CLIPS, KV_TOKENS, feature_width), jnp.float32), -6.0, 6.0)
    value_part = jnp.clip(jax.random.normal(key_list[6], (CLIPS, KV_TOKENS, feature_width), jnp.float32) * value_scale[:, None, None], -8.0, 8.0)
    key_values = jnp.concatenate([key_part, value_part], axis=2)
    return (queries, key_values)


def draw_q_student(key, part):
    return draw_pairs(jax.random.fold_in(key, 11), 0.0)[0].astype(jnp.bfloat16)


def draw_kv_student(key, part):
    return draw_pairs(jax.random.fold_in(key, 11), 0.0)[1].astype(jnp.bfloat16)


def draw_q_target(key, part):
    return draw_pairs(jax.random.fold_in(key, 23), 1.0)[0].astype(jnp.bfloat16)


def draw_kv_target(key, part):
    return draw_pairs(jax.random.fold_in(key, 23), 1.0)[1].astype(jnp.bfloat16)


def setup_inputs(seed: int = 0) -> dict:
    key_of = jax.random.split(jax.random.key(seed), 5)
    q_student = draw_q_student(jax.random.fold_in(key_of[4], 71), 0)
    kv_student = draw_kv_student(jax.random.fold_in(key_of[4], 71), 0)
    q_target = draw_q_target(jax.random.fold_in(key_of[4], 71), 0)
    kv_target = draw_kv_target(jax.random.fold_in(key_of[4], 71), 0)
    return dict(q_student=q_student, kv_student=kv_student, q_target=q_target, kv_target=kv_target)


def attend(queries, key_values):
    feature_width = HEADS * HD
    key_all = key_values[:, :feature_width].astype(jnp.float32).reshape(KV_TOKENS, HEADS, HD)
    value_all = key_values[:, feature_width:].astype(jnp.float32).reshape(KV_TOKENS, HEADS, HD)
    blocks = queries.reshape(N_SEQ, TOK_DEV, HEADS, HD)
    score_scale = 1.0 / (HD ** 0.5)

    def one_block(query_block):
        scores = jnp.einsum('qhd,khd->hqk', query_block.astype(jnp.float32), key_all) * score_scale
        row_max = jnp.max(scores, axis=-1, keepdims=True)
        exponent = jnp.exp(scores - row_max)
        row_total = jnp.sum(exponent, axis=-1)
        weights_bf = lax.optimization_barrier(exponent.astype(jnp.bfloat16)).astype(jnp.float32)
        mixed_rows = jnp.einsum('hqk,khd->hqd', weights_bf, value_all) / row_total[:, :, None]
        return jnp.transpose(mixed_rows, (1, 0, 2)).reshape(TOK_DEV, feature_width)

    return lax.map(one_block, blocks).reshape(TOKENS, feature_width)


def reference(q_student, kv_student, q_target, kv_target):
    student_rows = jnp.stack([attend(q_student[clip_index], kv_student[clip_index]) for clip_index in range(CLIPS)])
    target_rows = jnp.stack([attend(q_target[clip_index], kv_target[clip_index]) for clip_index in range(CLIPS)])
    position = jnp.arange(TOKENS).astype(jnp.float32)
    weight = 1.0 + 2.0 * position / float(max(TOKENS - 1, 1))
    gap_rows = student_rows - target_rows
    distill_loss = jnp.sum(weight[None, :, None] * gap_rows * gap_rows) / float(TOKENS * HEADS * HD)
    return student_rows.astype(jnp.bfloat16), target_rows.astype(jnp.bfloat16), distill_loss
```

```python
import functools

import jax
import jax.numpy as jnp
from jax import lax
from jax.experimental import pallas as pl
from jax.experimental.pallas import tpu as pltpu
from jax.sharding import PartitionSpec as P

HEADS = 12
HD = 128
FEAT = HEADS * HD
GROUPS = 3
WIDTH = FEAT // GROUPS
PAIR = 2 * HD
ROWS = 128
LOG2E = 1.4426950408889634
MESH = pl.DeviceIdType.MESH


def kernel(
    n, n_dp, q_s, kv_s, q_t, kv_t, out_s, out_t, loss_out,
    q_buf, k_buf, v_buf, loss_acc, loss_all,
    q_sem, own_sem, swap_s, swap_r, ay_s, ay_r, az_s, az_r, ap_s, ap_r,
    bz_s, bz_r, by_s, by_r, bp_s, bp_r, row_sem, loss_s, loss_r,
):
    line = n // 4
    me = lax.axis_index("seq")
    dp = lax.axis_index("dp")
    z, y, c = me // 4, (me // 2) % 2, me % 2
    partner = z * 4 + y * 2 + (1 - c)
    across = z * 4 + (1 - y) * 2 + c
    left, right = me - 4, me + 4

    def at(seq):
        return {"dp": dp, "seq": seq}

    own = []
    for m, ref in enumerate((kv_s, kv_t)):
        own.append(pltpu.make_async_copy(ref.at[0, :, pl.ds(0, FEAT)], k_buf.at[m, me], own_sem.at[m, 0]))
        own.append(pltpu.make_async_copy(ref.at[0, :, pl.ds(FEAT, FEAT)], v_buf.at[m, me], own_sem.at[m, 1]))
    for copy in own:
        copy.start()
    loads = [pltpu.make_async_copy(ref.at[0], q_buf.at[m], q_sem.at[m]) for m, ref in enumerate((q_s, q_t))]
    for copy in loads:
        copy.start()

    barrier = pltpu.get_barrier_semaphore()
    for seq in (partner, across):
        pl.semaphore_signal(barrier, inc=1, device_id=at(seq), device_id_type=MESH)
    for k in range(1, n_dp):
        pl.semaphore_signal(
            barrier, inc=1, device_id={"dp": (dp + k) % n_dp, "seq": me}, device_id_type=MESH
        )

    @pl.when(z > 0)
    def _():
        pl.semaphore_signal(barrier, inc=1, device_id=at(left), device_id_type=MESH)

    @pl.when(z < line - 1)
    def _():
        pl.semaphore_signal(barrier, inc=1, device_id=at(right), device_id_type=MESH)

    sides_here = jnp.where(z > 0, 1, 0) + jnp.where(z < line - 1, 1, 0)
    pl.semaphore_wait(barrier, 1 + n_dp + sides_here)

    for copy in own:
        copy.wait()

    def rdma(ref, send, recv, target):
        return pltpu.make_async_remote_copy(
            src_ref=ref, dst_ref=ref, send_sem=send, recv_sem=recv,
            device_id=at(target), device_id_type=MESH,
        )

    def cols(g):
        return pl.ds(g * WIDTH, WIDTH)

    def quad(g, zz):
        return k_buf.at[c, pl.ds(zz * 4, 4), :, cols(g)]

    def kpair(g, zz, yy, m):
        return k_buf.at[m, pl.ds(zz * 4 + yy * 2, 2), :, cols(g)]

    def vpair(g, zz, yy, m):
        return v_buf.at[m, pl.ds(zz * 4 + yy * 2, 2), :, cols(g)]

    def swap(g, m, part, dev):
        buf = (k_buf, v_buf)[part]
        return rdma(buf.at[m, dev, :, cols(g)], swap_s.at[g, m, part], swap_r.at[g, m, part], partner)

    def a_y(g, yy):
        return rdma(kpair(g, z, yy, c), ay_s.at[g], ay_r.at[g], across)

    def a_z(g, origin, slot, target):
        return rdma(quad(g, origin), az_s.at[g, slot], az_r.at[g, origin], target)

    def a_p(g, origin, m):
        ref = k_buf.at[m, pl.ds(origin * 4, 4), :, cols(g)]
        return rdma(ref, ap_s.at[g, origin], ap_r.at[g, origin], partner)

    def a_py(g, m):
        return rdma(kpair(g, z, 1 - y, m), ap_s.at[g, z], ap_r.at[g, z], partner)

    def b_z(g, origin, slot, target):
        return rdma(vpair(g, origin, y, c), bz_s.at[g, slot], bz_r.at[g, origin], target)

    def b_y(g, origin, yy):
        return rdma(vpair(g, origin, yy, c), by_s.at[g, origin], by_r.at[g, origin], across)

    def b_p(g, origin, yy, flag, m):
        return rdma(vpair(g, origin, yy, m), bp_s.at[g, flag, origin], bp_r.at[g, flag, origin], partner)

    def sides(s, act):
        @pl.when(z - s >= 0)
        def _():
            act(z - s, z + 1 < line, right)

        @pl.when(z + s < line)
        def _():
            act(z + s, z > 0, left)

    def ends(make_copy):
        @pl.when(z + 1 < line)
        def _():
            make_copy(z, right)

        @pl.when(z > 0)
        def _():
            make_copy(line, left)

    def stage(g, t):
        if t == 0:
            for part in range(2):
                for m in range(2):
                    swap(g, m, part, partner).wait_recv()
            a_y(g, y).start()
            ends(lambda slot, target: b_z(g, z, slot, target).start())
            b_y(g, z, y).start()
        if t == 1:
            a_y(g, 1 - y).wait_recv()
            ends(lambda slot, target: a_z(g, z, slot, target).start())
            a_py(g, c).start()
        if 1 <= t < line:
            def act(origin, more, target):
                b_z(g, origin, origin, target).wait_recv()

                @pl.when(more)
                def _():
                    b_z(g, origin, origin, target).start()

                b_y(g, origin, y).start()
                b_p(g, origin, y, 0, c).start()

            sides(t, act)
        if t == 1:
            b_y(g, z, 1 - y).wait_recv()
            b_p(g, z, 1 - y, 1, c).start()
        if 2 <= t <= line:
            def act2(origin, more, target):
                a_z(g, origin, origin, target).wait_recv()

                @pl.when(more)
                def _():
                    a_z(g, origin, origin, target).start()

                a_p(g, origin, c).start()
                b_y(g, origin, 1 - y).wait_recv()
                b_p(g, origin, 1 - y, 1, c).start()

            sides(t - 1, act2)
        if t == line + 1:
            a_py(g, 1 - c).wait_recv()
            b_p(g, z, 1 - y, 1, 1 - c).wait_recv()
            for s in range(1, line):
                def act3(origin, more, target):
                    a_p(g, origin, 1 - c).wait_recv()
                    b_p(g, origin, y, 0, 1 - c).wait_recv()
                    b_p(g, origin, 1 - y, 1, 1 - c).wait_recv()

                sides(s, act3)

    def drain(g):
        for part in range(2):
            for m in range(2):
                swap(g, m, part, me).wait_send()
        a_y(g, y).wait_send()
        a_py(g, c).wait_send()
        b_y(g, z, y).wait_send()
        b_p(g, z, 1 - y, 1, c).wait_send()
        ends(lambda slot, target: a_z(g, z, slot, target).wait_send())
        ends(lambda slot, target: b_z(g, z, slot, target).wait_send())
        for s in range(1, line):
            def act(origin, more, target):
                @pl.when(more)
                def _():
                    a_z(g, origin, origin, target).wait_send()
                    b_z(g, origin, origin, target).wait_send()

                a_p(g, origin, c).wait_send()
                b_y(g, origin, y).wait_send()
                b_p(g, origin, y, 0, c).wait_send()
                b_p(g, origin, 1 - y, 1, c).wait_send()

            sides(s, act)

    keys = n * 8
    rows = q_buf.shape[1]
    total_rows = rows * n
    factor = LOG2E / HD**0.5

    def head_block(buf, m, col):
        block = buf[m, :, :, pl.ds(col, HD)].astype(jnp.float32)
        return block.reshape(keys, HD).astype(jnp.bfloat16)

    def paired(buf, m, col):
        zero = jnp.zeros((keys, HD), jnp.bfloat16)
        top = jnp.concatenate([head_block(buf, m, col), zero], axis=1)
        low = jnp.concatenate([zero, head_block(buf, m, col + HD)], axis=1)
        return jnp.concatenate([top, low], axis=0)

    def compute(g):
        for pair in range(WIDTH // PAIR):
            col = g * WIDTH + pair * PAIR
            mats = [(paired(k_buf, m, col), paired(v_buf, m, col)) for m in range(2)]

            def tile(i, carry):
                base = pl.multiple_of(i * ROWS, ROWS)
                span = pl.ds(base, ROWS)
                mixed = []
                for m in range(2):
                    key2, value2 = mats[m]
                    scores = lax.dot_general(
                        q_buf[m, span, pl.ds(col, PAIR)], key2, (((1,), (1,)), ((), ())),
                        preferred_element_type=jnp.float32,
                    )
                    expo, inverse = [], []
                    for h in range(2):
                        part = scores[:, h * keys : (h + 1) * keys]
                        top = jnp.max(part, axis=-1, keepdims=True)
                        e = jnp.exp2((part - top) * factor)
                        inverse.append(1.0 / jnp.sum(e, axis=-1, keepdims=True))
                        expo.append(e.astype(jnp.bfloat16))
                    out = jnp.dot(
                        jnp.concatenate(expo, axis=1), value2, preferred_element_type=jnp.float32
                    )
                    mixed.append([out[:, h * HD : (h + 1) * HD] * inverse[h] for h in range(2)])
                for m, ref in enumerate((out_s, out_t)):
                    for h in range(2):
                        ref[0, span, pl.ds(col + h * HD, HD)] = mixed[m][h].astype(jnp.bfloat16)
                position = me * rows + base + lax.broadcasted_iota(jnp.int32, (ROWS, HD), 0)
                weight = 1.0 + position.astype(jnp.float32) * (2.0 / max(total_rows - 1, 1))
                gap0 = mixed[0][0] - mixed[1][0]
                gap1 = mixed[0][1] - mixed[1][1]
                term = weight * (gap0 * gap0 + gap1 * gap1)
                loss_acc[...] += jnp.sum(term.reshape(ROWS // 8, 8, HD), axis=0)
                return carry

            lax.fori_loop(0, rows // ROWS, tile, 0, unroll=2)

    loss_acc[...] = jnp.zeros_like(loss_acc)
    for g in range(GROUPS):
        for part in range(2):
            for m in range(2):
                swap(g, m, part, me).start()
    last = line + 1
    for t in range(last + GROUPS):
        for g in range(GROUPS):
            if 0 <= t - g <= last:
                stage(g, t - g)
        if t == last:
            for k in range(1, n_dp):
                pl.semaphore_signal(
                    row_sem, inc=1, device_id={"dp": (dp + k) % n_dp, "seq": me}, device_id_type=MESH
                )
            for copy in loads:
                copy.wait()
        if t >= last:
            compute(t - last)

    flat = dp * n + me
    count = n * n_dp
    loss_all[flat] = jnp.sum(loss_acc[...], axis=0, keepdims=True)
    pl.semaphore_wait(row_sem, n_dp - 1)

    def exchange(source, k, target):
        return pltpu.make_async_remote_copy(
            src_ref=loss_all.at[source], dst_ref=loss_all.at[source],
            send_sem=loss_s.at[k], recv_sem=loss_r.at[k],
            device_id={"dp": target // n, "seq": target % n}, device_id_type=MESH,
        )

    def send(k, carry):
        exchange(flat, k, (flat + k) % count).start()
        return carry

    lax.fori_loop(1, count, send, 0)
    for g in range(GROUPS):
        drain(g)

    def receive(k, carry):
        target = (flat + k) % count
        exchange((flat + count - k) % count, k, target).wait_recv()
        exchange(flat, k, target).wait_send()
        return carry

    lax.fori_loop(1, count, receive, 0)
    total = jnp.sum(loss_all[...]) / float(total_rows * FEAT)
    loss_out[0, 0] = total


def body(n, n_dp, q_student, kv_student, q_target, kv_target):
    rows = q_student.shape[1]
    line = n // 4
    dma = pltpu.SemaphoreType.DMA
    any_spec = pl.BlockSpec(memory_space=pl.ANY)
    vmem_spec = pl.BlockSpec(memory_space=pltpu.VMEM)
    outs = pl.pallas_call(
        functools.partial(kernel, n, n_dp),
        out_shape=(
            jax.ShapeDtypeStruct(q_student.shape, jnp.bfloat16),
            jax.ShapeDtypeStruct(q_student.shape, jnp.bfloat16),
            jax.ShapeDtypeStruct((1, 1), jnp.float32),
        ),
        in_specs=[any_spec] * 4,
        out_specs=(vmem_spec, vmem_spec, pl.BlockSpec(memory_space=pltpu.SMEM)),
        scratch_shapes=[
            pltpu.VMEM((2, rows, FEAT), jnp.bfloat16),
            pltpu.VMEM((2, n, 8, FEAT), jnp.bfloat16),
            pltpu.VMEM((2, n, 8, FEAT), jnp.bfloat16),
            pltpu.VMEM((8, HD), jnp.float32),
            pltpu.VMEM((n * n_dp, 1, HD), jnp.float32),
            dma((2,)),
            dma((2, 2)),
            dma((GROUPS, 2, 2)),
            dma((GROUPS, 2, 2)),
            dma((GROUPS,)),
            dma((GROUPS,)),
            dma((GROUPS, line + 1)),
            dma((GROUPS, line)),
            dma((GROUPS, line)),
            dma((GROUPS, line)),
            dma((GROUPS, line + 1)),
            dma((GROUPS, line)),
            dma((GROUPS, line)),
            dma((GROUPS, line)),
            dma((GROUPS, 2, line)),
            dma((GROUPS, 2, line)),
            pltpu.SemaphoreType.REGULAR,
            dma((n * n_dp,)),
            dma((n * n_dp,)),
        ],
        compiler_params=pltpu.CompilerParams(
            collective_id=0, has_side_effects=True, vmem_limit_bytes=60 * 1024 * 1024
        ),
    )(q_student, kv_student, q_target, kv_target)
    return outs[0], outs[1], outs[2].reshape(())


def solution(mesh):
    n, n_dp = mesh.shape["seq"], mesh.shape["dp"]
    spec = P("dp", "seq", None)
    return jax.shard_map(
        functools.partial(body, n, n_dp),
        mesh=mesh,
        in_specs=(spec,) * 4,
        out_specs=(spec, spec, P()),
        check_vma=False,
    )
```

```python
import functools

import jax
import jax.numpy as jnp
from jax import lax
from jax.experimental import pallas as pl
from jax.experimental.pallas import tpu as pltpu
from jax.sharding import PartitionSpec as P

HEADS = 12
HD = 128
FEAT = HEADS * HD
GROUPS = 1
WIDTH = FEAT // GROUPS
PAIR = 2 * HD
ROWS = 128
LOG2E = 1.4426950408889634
MESH = pl.DeviceIdType.MESH


def kernel(
    n, n_dp, q_s, kv_s, q_t, kv_t, out_s, out_t, loss_out,
    q_buf, k_buf, v_buf, loss_acc, loss_all,
    q_sem, own_sem, swap_s, swap_r, ay_s, ay_r, az_s, az_r, ap_s, ap_r,
    bz_s, bz_r, by_s, by_r, bp_s, bp_r, row_sem, loss_s, loss_r,
):
    line = n // 4
    me = lax.axis_index("seq")
    dp = lax.axis_index("dp")
    z, y, c = me // 4, (me // 2) % 2, me % 2
    partner = z * 4 + y * 2 + (1 - c)
    across = z * 4 + (1 - y) * 2 + c
    left, right = me - 4, me + 4

    def at(seq):
        return {"dp": dp, "seq": seq}

    own = []
    for m, ref in enumerate((kv_s, kv_t)):
        own.append(pltpu.make_async_copy(ref.at[0, :, pl.ds(0, FEAT)], k_buf.at[m, me], own_sem.at[m, 0]))
        own.append(pltpu.make_async_copy(ref.at[0, :, pl.ds(FEAT, FEAT)], v_buf.at[m, me], own_sem.at[m, 1]))
    for copy in own:
        copy.start()
    loads = [pltpu.make_async_copy(ref.at[0], q_buf.at[m], q_sem.at[m]) for m, ref in enumerate((q_s, q_t))]
    for copy in loads:
        copy.start()

    barrier = pltpu.get_barrier_semaphore()
    for seq in (partner, across):
        pl.semaphore_signal(barrier, inc=1, device_id=at(seq), device_id_type=MESH)
    for k in range(1, n_dp):
        pl.semaphore_signal(
            barrier, inc=1, device_id={"dp": (dp + k) % n_dp, "seq": me}, device_id_type=MESH
        )

    @pl.when(z > 0)
    def _():
        pl.semaphore_signal(barrier, inc=1, device_id=at(left), device_id_type=MESH)

    @pl.when(z < line - 1)
    def _():
        pl.semaphore_signal(barrier, inc=1, device_id=at(right), device_id_type=MESH)

    sides_here = jnp.where(z > 0, 1, 0) + jnp.where(z < line - 1, 1, 0)
    pl.semaphore_wait(barrier, 1 + n_dp + sides_here)

    for copy in own:
        copy.wait()

    def rdma(ref, send, recv, target):
        return pltpu.make_async_remote_copy(
            src_ref=ref, dst_ref=ref, send_sem=send, recv_sem=recv,
            device_id=at(target), device_id_type=MESH,
        )

    def cols(g):
        return pl.ds(g * WIDTH, WIDTH)

    def quad(g, zz):
        return k_buf.at[c, pl.ds(zz * 4, 4), :, cols(g)]

    def kpair(g, zz, yy, m):
        return k_buf.at[m, pl.ds(zz * 4 + yy * 2, 2), :, cols(g)]

    def vpair(g, zz, yy, m):
        return v_buf.at[m, pl.ds(zz * 4 + yy * 2, 2), :, cols(g)]

    def swap(g, m, part, dev):
        buf = (k_buf, v_buf)[part]
        return rdma(buf.at[m, dev, :, cols(g)], swap_s.at[g, m, part], swap_r.at[g, m, part], partner)

    def a_y(g, yy):
        return rdma(kpair(g, z, yy, c), ay_s.at[g], ay_r.at[g], across)

    def a_z(g, origin, slot, target):
        return rdma(quad(g, origin), az_s.at[g, slot], az_r.at[g, origin], target)

    def a_p(g, origin, m):
        ref = k_buf.at[m, pl.ds(origin * 4, 4), :, cols(g)]
        return rdma(ref, ap_s.at[g, origin], ap_r.at[g, origin], partner)

    def a_py(g, m):
        return rdma(kpair(g, z, 1 - y, m), ap_s.at[g, z], ap_r.at[g, z], partner)

    def b_z(g, origin, slot, target):
        return rdma(vpair(g, origin, y, c), bz_s.at[g, slot], bz_r.at[g, origin], target)

    def b_y(g, origin, yy):
        return rdma(vpair(g, origin, yy, c), by_s.at[g, origin], by_r.at[g, origin], across)

    def b_p(g, origin, yy, flag, m):
        return rdma(vpair(g, origin, yy, m), bp_s.at[g, flag, origin], bp_r.at[g, flag, origin], partner)

    def sides(s, act):
        @pl.when(z - s >= 0)
        def _():
            act(z - s, z + 1 < line, right)

        @pl.when(z + s < line)
        def _():
            act(z + s, z > 0, left)

    def ends(make_copy):
        @pl.when(z + 1 < line)
        def _():
            make_copy(z, right)

        @pl.when(z > 0)
        def _():
            make_copy(line, left)

    def stage(g, t):
        if t == 0:
            for part in range(2):
                for m in range(2):
                    swap(g, m, part, partner).wait_recv()
            a_y(g, y).start()
            ends(lambda slot, target: b_z(g, z, slot, target).start())
            b_y(g, z, y).start()
        if t == 1:
            a_y(g, 1 - y).wait_recv()
            ends(lambda slot, target: a_z(g, z, slot, target).start())
            a_py(g, c).start()
        if 1 <= t < line:
            def act(origin, more, target):
                b_z(g, origin, origin, target).wait_recv()

                @pl.when(more)
                def _():
                    b_z(g, origin, origin, target).start()

                b_y(g, origin, y).start()
                b_p(g, origin, y, 0, c).start()

            sides(t, act)
        if t == 1:
            b_y(g, z, 1 - y).wait_recv()
            b_p(g, z, 1 - y, 1, c).start()
        if 2 <= t <= line:
            def act2(origin, more, target):
                a_z(g, origin, origin, target).wait_recv()

                @pl.when(more)
                def _():
                    a_z(g, origin, origin, target).start()

                a_p(g, origin, c).start()
                b_y(g, origin, 1 - y).wait_recv()
                b_p(g, origin, 1 - y, 1, c).start()

            sides(t - 1, act2)
        if t == line + 1:
            a_py(g, 1 - c).wait_recv()
            b_p(g, z, 1 - y, 1, 1 - c).wait_recv()
            for s in range(1, line):
                def act3(origin, more, target):
                    a_p(g, origin, 1 - c).wait_recv()
                    b_p(g, origin, y, 0, 1 - c).wait_recv()
                    b_p(g, origin, 1 - y, 1, 1 - c).wait_recv()

                sides(s, act3)

    def drain(g):
        for part in range(2):
            for m in range(2):
                swap(g, m, part, me).wait_send()
        a_y(g, y).wait_send()
        a_py(g, c).wait_send()
        b_y(g, z, y).wait_send()
        b_p(g, z, 1 - y, 1, c).wait_send()
        ends(lambda slot, target: a_z(g, z, slot, target).wait_send())
        ends(lambda slot, target: b_z(g, z, slot, target).wait_send())
        for s in range(1, line):
            def act(origin, more, target):
                @pl.when(more)
                def _():
                    a_z(g, origin, origin, target).wait_send()
                    b_z(g, origin, origin, target).wait_send()

                a_p(g, origin, c).wait_send()
                b_y(g, origin, y).wait_send()
                b_p(g, origin, y, 0, c).wait_send()
                b_p(g, origin, 1 - y, 1, c).wait_send()

            sides(s, act)

    keys = n * 8
    rows = q_buf.shape[1]
    total_rows = rows * n
    factor = LOG2E / HD**0.5

    def head_block(buf, m, col):
        block = buf[m, :, :, pl.ds(col, HD)].astype(jnp.float32)
        return block.reshape(keys, HD).astype(jnp.bfloat16)

    def paired(buf, m, col):
        zero = jnp.zeros((keys, HD), jnp.bfloat16)
        top = jnp.concatenate([head_block(buf, m, col), zero], axis=1)
        low = jnp.concatenate([zero, head_block(buf, m, col + HD)], axis=1)
        return jnp.concatenate([top, low], axis=0)

    def compute(g):
        for pair in range(WIDTH // PAIR):
            col = g * WIDTH + pair * PAIR
            mats = [(paired(k_buf, m, col), paired(v_buf, m, col)) for m in range(2)]

            def tile(i, carry):
                base = pl.multiple_of(i * ROWS, ROWS)
                span = pl.ds(base, ROWS)
                mixed = []
                for m in range(2):
                    key2, value2 = mats[m]
                    scores = lax.dot_general(
                        q_buf[m, span, pl.ds(col, PAIR)], key2, (((1,), (1,)), ((), ())),
                        preferred_element_type=jnp.float32,
                    )
                    expo, inverse = [], []
                    for h in range(2):
                        part = scores[:, h * keys : (h + 1) * keys]
                        top = jnp.max(part, axis=-1, keepdims=True)
                        e = jnp.exp2((part - top) * factor)
                        inverse.append(1.0 / jnp.sum(e, axis=-1, keepdims=True))
                        expo.append(e.astype(jnp.bfloat16))
                    out = jnp.dot(
                        jnp.concatenate(expo, axis=1), value2, preferred_element_type=jnp.float32
                    )
                    mixed.append([out[:, h * HD : (h + 1) * HD] * inverse[h] for h in range(2)])
                for m, ref in enumerate((out_s, out_t)):
                    for h in range(2):
                        ref[0, span, pl.ds(col + h * HD, HD)] = mixed[m][h].astype(jnp.bfloat16)
                position = me * rows + base + lax.broadcasted_iota(jnp.int32, (ROWS, HD), 0)
                weight = 1.0 + position.astype(jnp.float32) * (2.0 / max(total_rows - 1, 1))
                gap0 = mixed[0][0] - mixed[1][0]
                gap1 = mixed[0][1] - mixed[1][1]
                term = weight * (gap0 * gap0 + gap1 * gap1)
                loss_acc[...] += jnp.sum(term.reshape(ROWS // 8, 8, HD), axis=0)
                return carry

            lax.fori_loop(0, rows // ROWS, tile, 0, unroll=2)

    loss_acc[...] = jnp.zeros_like(loss_acc)
    for g in range(GROUPS):
        for part in range(2):
            for m in range(2):
                swap(g, m, part, me).start()
    last = line + 1
    for t in range(last + GROUPS):
        for g in range(GROUPS):
            if 0 <= t - g <= last:
                stage(g, t - g)
        if t == last:
            for k in range(1, n_dp):
                pl.semaphore_signal(
                    row_sem, inc=1, device_id={"dp": (dp + k) % n_dp, "seq": me}, device_id_type=MESH
                )
            for copy in loads:
                copy.wait()
        if t >= last:
            compute(t - last)

    flat = dp * n + me
    count = n * n_dp
    loss_all[flat] = jnp.sum(loss_acc[...], axis=0, keepdims=True)
    pl.semaphore_wait(row_sem, n_dp - 1)

    def exchange(source, k, target):
        return pltpu.make_async_remote_copy(
            src_ref=loss_all.at[source], dst_ref=loss_all.at[source],
            send_sem=loss_s.at[k], recv_sem=loss_r.at[k],
            device_id={"dp": target // n, "seq": target % n}, device_id_type=MESH,
        )

    def send(k, carry):
        exchange(flat, k, (flat + k) % count).start()
        return carry

    lax.fori_loop(1, count, send, 0)
    for g in range(GROUPS):
        drain(g)

    def receive(k, carry):
        target = (flat + k) % count
        exchange((flat + count - k) % count, k, target).wait_recv()
        exchange(flat, k, target).wait_send()
        return carry

    lax.fori_loop(1, count, receive, 0)
    total = jnp.sum(loss_all[...]) / float(total_rows * FEAT)
    loss_out[0, 0] = total


def body(n, n_dp, q_student, kv_student, q_target, kv_target):
    rows = q_student.shape[1]
    line = n // 4
    dma = pltpu.SemaphoreType.DMA
    any_spec = pl.BlockSpec(memory_space=pl.ANY)
    vmem_spec = pl.BlockSpec(memory_space=pltpu.VMEM)
    outs = pl.pallas_call(
        functools.partial(kernel, n, n_dp),
        out_shape=(
            pltpu.VMEM(q_student.shape, jnp.bfloat16),
            pltpu.VMEM(q_student.shape, jnp.bfloat16),
            jax.ShapeDtypeStruct((1, 1), jnp.float32),
        ),
        in_specs=[any_spec] * 4,
        out_specs=(vmem_spec, vmem_spec, pl.BlockSpec(memory_space=pltpu.SMEM)),
        scratch_shapes=[
            pltpu.VMEM((2, rows, FEAT), jnp.bfloat16),
            pltpu.VMEM((2, n, 8, FEAT), jnp.bfloat16),
            pltpu.VMEM((2, n, 8, FEAT), jnp.bfloat16),
            pltpu.VMEM((8, HD), jnp.float32),
            pltpu.VMEM((n * n_dp, 1, HD), jnp.float32),
            dma((2,)),
            dma((2, 2)),
            dma((GROUPS, 2, 2)),
            dma((GROUPS, 2, 2)),
            dma((GROUPS,)),
            dma((GROUPS,)),
            dma((GROUPS, line + 1)),
            dma((GROUPS, line)),
            dma((GROUPS, line)),
            dma((GROUPS, line)),
            dma((GROUPS, line + 1)),
            dma((GROUPS, line)),
            dma((GROUPS, line)),
            dma((GROUPS, line)),
            dma((GROUPS, 2, line)),
            dma((GROUPS, 2, line)),
            pltpu.SemaphoreType.REGULAR,
            dma((n * n_dp,)),
            dma((n * n_dp,)),
        ],
        compiler_params=pltpu.CompilerParams(
            collective_id=0, has_side_effects=True, vmem_limit_bytes=60 * 1024 * 1024
        ),
    )(q_student, kv_student, q_target, kv_target)
    return outs[0], outs[1], outs[2].reshape(())


def solution(mesh):
    n, n_dp = mesh.shape["seq"], mesh.shape["dp"]
    spec = P("dp", "seq", None)
    return jax.shard_map(
        functools.partial(body, n, n_dp),
        mesh=mesh,
        in_specs=(spec,) * 4,
        out_specs=(spec, spec, P()),
        check_vma=False,
    )
```

```python
import functools

import jax
import jax.numpy as jnp
from jax import lax
from jax.experimental import pallas as pl
from jax.experimental.pallas import tpu as pltpu
from jax.sharding import PartitionSpec as P

HEADS = 12
HD = 128
FEAT = HEADS * HD
GROUPS = 3
WIDTH = FEAT // GROUPS
PAIR = 2 * HD
ROWS = 256
LOG2E = 1.4426950408889634
MESH = pl.DeviceIdType.MESH


def kernel(
    n, n_dp, q_s, kv_s, q_t, kv_t, out_s, out_t, loss_out,
    q_buf, buf, loss_acc, loss_all,
    q_sem, own_sem, swap_s, swap_r, z_s, z_r, y_s, y_r, p_s, p_r, row_sem, loss_s, loss_r,
):
    line = n // 4
    me = lax.axis_index("seq")
    dp = lax.axis_index("dp")
    z, y, c = me // 4, (me // 2) % 2, me % 2
    partner = z * 4 + y * 2 + (1 - c)
    across = z * 4 + (1 - y) * 2 + c

    def at(seq):
        return {"dp": dp, "seq": seq}

    def plane(k):
        return (z + k) % line

    own = [
        pltpu.make_async_copy(
            ref.at[0, :, pl.ds(part * FEAT + g * WIDTH, WIDTH)],
            buf.at[m, g, me, part],
            own_sem.at[m, g, part],
        )
        for g in range(GROUPS)
        for m, ref in enumerate((kv_s, kv_t))
        for part in range(2)
    ]
    for copy in own:
        copy.start()
    loads = [pltpu.make_async_copy(ref.at[0], q_buf.at[m], q_sem.at[m]) for m, ref in enumerate((q_s, q_t))]
    for copy in loads:
        copy.start()

    barrier = pltpu.get_barrier_semaphore()
    first = [at(partner), at(across)]
    first += [at(plane(k) * 4 + y * 2 + c) for k in range(1, line)]
    first += [{"dp": (dp + k) % n_dp, "seq": me} for k in range(1, n_dp)]
    for device in first:
        pl.semaphore_signal(barrier, inc=1, device_id=device, device_id_type=MESH)
    pl.semaphore_wait(barrier, len(first))

    for copy in own:
        copy.wait()

    def rdma(ref, send, recv, target):
        return pltpu.make_async_remote_copy(
            src_ref=ref, dst_ref=ref, send_sem=send, recv_sem=recv,
            device_id=at(target), device_id_type=MESH,
        )

    def duo(m, g, zz, yy):
        return buf.at[m, g, pl.ds(zz * 4 + yy * 2, 2)]

    def swap(g, m, dev):
        return rdma(buf.at[m, g, dev], swap_s.at[g, m], swap_r.at[g, m], partner)

    def along(g, k, origin):
        return rdma(duo(c, g, origin, y), z_s.at[g, k], z_r.at[g, k], plane(k) * 4 + y * 2 + c)

    def over(g, k, yy):
        return rdma(duo(c, g, plane(line - k), yy), y_s.at[g, k], y_r.at[g, k], across)

    def share(g, k, side, m):
        yy = y if side == 0 else 1 - y
        ref = duo(m, g, plane(line - k), yy)
        return rdma(ref, p_s.at[g, side, k], p_r.at[g, side, k], partner)

    def relay_z(g):
        for k in range(1, line):
            along(g, k, plane(line - k)).wait_recv()
            over(g, k, y).start()
            share(g, k, 0, c).start()

    def relay_y(g):
        for k in range(line):
            over(g, k, 1 - y).wait_recv()
            share(g, k, 1, c).start()

    def finish(g):
        for k in range(line):
            if k:
                share(g, k, 0, 1 - c).wait_recv()
            share(g, k, 1, 1 - c).wait_recv()

    def drain(g):
        for m in range(2):
            swap(g, m, me).wait_send()
        for k in range(line):
            over(g, k, y).wait_send()
            share(g, k, 1, c).wait_send()
            if k:
                along(g, k, z).wait_send()
                share(g, k, 0, c).wait_send()

    keys = n * 8
    rows = q_buf.shape[1]
    total_rows = rows * n
    factor = LOG2E / HD**0.5

    def head_block(m, g, part, col):
        block = buf[m, g, :, part, :, pl.ds(col, HD)].astype(jnp.float32)
        return block.reshape(keys, HD).astype(jnp.bfloat16)

    def paired(m, g, part, col):
        zero = jnp.zeros((keys, HD), jnp.bfloat16)
        top = jnp.concatenate([head_block(m, g, part, col), zero], axis=1)
        low = jnp.concatenate([zero, head_block(m, g, part, col + HD)], axis=1)
        return jnp.concatenate([top, low], axis=0)

    def compute(g, pair):
            col = g * WIDTH + pair * PAIR
            mats = [
                (paired(m, g, 0, pair * PAIR), paired(m, g, 1, pair * PAIR)) for m in range(2)
            ]

            def tile(i, carry):
                base = i * ROWS
                span = pl.ds(base, ROWS)
                mixed = []
                for m in range(2):
                    key2, value2 = mats[m]
                    scores = lax.dot_general(
                        q_buf[m, span, pl.ds(col, PAIR)], key2, (((1,), (1,)), ((), ())),
                        preferred_element_type=jnp.float32,
                    )
                    expo, inverse = [], []
                    for h in range(2):
                        part = scores[:, h * keys : (h + 1) * keys]
                        top = jnp.max(part, axis=-1, keepdims=True)
                        e = jnp.exp2((part - top) * factor)
                        inverse.append(1.0 / jnp.sum(e, axis=-1, keepdims=True))
                        expo.append(e.astype(jnp.bfloat16))
                    out = jnp.dot(
                        jnp.concatenate(expo, axis=1), value2, preferred_element_type=jnp.float32
                    )
                    mixed.append([out[:, h * HD : (h + 1) * HD] * inverse[h] for h in range(2)])
                for m, ref in enumerate((out_s, out_t)):
                    for h in range(2):
                        ref[0, span, pl.ds(col + h * HD, HD)] = mixed[m][h].astype(jnp.bfloat16)
                position = me * rows + base + lax.broadcasted_iota(jnp.int32, (ROWS, HD), 0)
                weight = 1.0 + position.astype(jnp.float32) * (2.0 / max(total_rows - 1, 1))
                gap0 = mixed[0][0] - mixed[1][0]
                gap1 = mixed[0][1] - mixed[1][1]
                term = weight * (gap0 * gap0 + gap1 * gap1)
                loss_acc[...] += jnp.sum(term.reshape(ROWS // 8, 8, HD), axis=0)
                return carry

            for i in range(rows // ROWS):
                tile(i, 0)

    loss_acc[...] = jnp.zeros_like(loss_acc)
    for g in range(GROUPS):
        for m in range(2):
            swap(g, m, me).start()
    for g in range(GROUPS):
        for m in range(2):
            swap(g, m, partner).wait_recv()
        for k in range(1, line):
            along(g, k, z).start()
        over(g, 0, y).start()
    relay_z(0)
    if GROUPS > 1:
        relay_z(1)
    relay_y(0)
    finish(0)
    for k in range(1, n_dp):
        pl.semaphore_signal(
            row_sem, inc=1, device_id={"dp": (dp + k) % n_dp, "seq": me}, device_id_type=MESH
        )
    for copy in loads:
        copy.wait()
    pairs = WIDTH // PAIR
    for g in range(GROUPS):
        for pair in range(pairs):
            if pair == pairs - 1 and g + 1 < GROUPS:
                relay_y(g + 1)
                if g + 2 < GROUPS:
                    relay_z(g + 2)
            compute(g, pair)
        if g + 1 < GROUPS:
            finish(g + 1)

    flat = dp * n + me
    count = n * n_dp
    loss_all[flat] = jnp.sum(loss_acc[...], axis=0, keepdims=True)
    pl.semaphore_wait(row_sem, n_dp - 1)

    def exchange(source, k, target):
        return pltpu.make_async_remote_copy(
            src_ref=loss_all.at[source], dst_ref=loss_all.at[source],
            send_sem=loss_s.at[k], recv_sem=loss_r.at[k],
            device_id={"dp": target // n, "seq": target % n}, device_id_type=MESH,
        )

    def send(k, carry):
        exchange(flat, k, (flat + k) % count).start()
        return carry

    lax.fori_loop(1, count, send, 0)
    for g in range(GROUPS):
        drain(g)

    def receive(k, carry):
        target = (flat + k) % count
        exchange((flat + count - k) % count, k, target).wait_recv()
        exchange(flat, k, target).wait_send()
        return carry

    lax.fori_loop(1, count, receive, 0)
    total = jnp.sum(loss_all[...]) / float(total_rows * FEAT)
    loss_out[0, 0] = total


def body(n, n_dp, q_student, kv_student, q_target, kv_target):
    rows = q_student.shape[1]
    line = n // 4
    dma = pltpu.SemaphoreType.DMA
    any_spec = pl.BlockSpec(memory_space=pl.ANY)
    vmem_spec = pl.BlockSpec(memory_space=pltpu.VMEM)
    outs = pl.pallas_call(
        functools.partial(kernel, n, n_dp),
        out_shape=(
            pltpu.VMEM(q_student.shape, jnp.bfloat16),
            pltpu.VMEM(q_student.shape, jnp.bfloat16),
            jax.ShapeDtypeStruct((1, 1), jnp.float32),
        ),
        in_specs=[any_spec] * 4,
        out_specs=(vmem_spec, vmem_spec, pl.BlockSpec(memory_space=pltpu.SMEM)),
        scratch_shapes=[
            pltpu.VMEM((2, rows, FEAT), jnp.bfloat16),
            pltpu.VMEM((2, GROUPS, n, 2, 8, WIDTH), jnp.bfloat16),
            pltpu.VMEM((8, HD), jnp.float32),
            pltpu.VMEM((n * n_dp, 1, HD), jnp.float32),
            dma((2,)),
            dma((2, GROUPS, 2)),
            dma((GROUPS, 2)),
            dma((GROUPS, 2)),
            dma((GROUPS, line)),
            dma((GROUPS, line)),
            dma((GROUPS, line)),
            dma((GROUPS, line)),
            dma((GROUPS, 2, line)),
            dma((GROUPS, 2, line)),
            pltpu.SemaphoreType.REGULAR,
            dma((n * n_dp,)),
            dma((n * n_dp,)),
        ],
        compiler_params=pltpu.CompilerParams(
            collective_id=0, has_side_effects=True, vmem_limit_bytes=60 * 1024 * 1024
        ),
    )(q_student, kv_student, q_target, kv_target)
    return outs[0], outs[1], outs[2].reshape(())


def solution(mesh):
    n, n_dp = mesh.shape["seq"], mesh.shape["dp"]
    spec = P("dp", "seq", None)
    return jax.shard_map(
        functools.partial(body, n, n_dp),
        mesh=mesh,
        in_specs=(spec,) * 4,
        out_specs=(spec, spec, P()),
        check_vma=False,
    )
```
